32 devices in a mesh: row: 8 (over y, x, core), col: 4 (over z).
Axes of the slice: x: 2, y: 2, z: 4, core: 2. Of those that a mesh axis runs over, the one named last changes fastest.
Arguments:
- schur_tail: float32 [1024, 1024], P(('row', 'col')), as said below
- coupling: float32 [1024, 16384], P(None, 'row'), may hold values from -4 to 4
- ks_lead: float32 [16384, 4096], P('row', 'col'), may hold values from -0.046875 to 0.046875
- ks_tail: float32 [1024, 4096], P('row', 'col'), may hold values from -0.046875 to 0.046875
- inv_mask: int32 [8, 136], replicated, may hold values 0 or 1
- ks_mask: int32 [136, 32], replicated, may hold values 0 or 1
Outputs:
- projected: float32 [1024, 4096], P('row', 'col')
The draws below stay inside these ranges and needn't reach their ends.
Inputs may be any that keep to these rules, and one draw needn't show every extreme that they name: `schur_tail`: symmetric and positive definite, with diagonal entries between about 1 and 32.
All inputs are finite; a program needn't handle non-finite values.
Results may differ from the reference program's by a relative error of at most 0.00009.
Values sent between devices are 32-bit elements; how exact they have to be, the bound alone decides.
A program may use at most 128 MiB of HBM per device.

```python
import math
import jax
import jax.numpy as jnp
from jax import lax

NL = 16384
BLK = 128
NC = 4096
K = 1024
N = 17408


def draw_schur_tail(key, part):
    key_one = jax.random.fold_in(key, 0)
    key_two = jax.random.fold_in(key, 1)
    key_four = jax.random.fold_in(key, 3)
    entries = jax.random.normal(key_one, (K, K), jnp.float32) * (0.8 / math.sqrt(2.0 * K))
    symmetric = (entries + entries.T) * 0.5
    diagonal_part = jax.random.uniform(key_two, (K,), jnp.float32, 1.0, 2.0)
    vector = jax.random.uniform(key_four, (K,), jnp.float32, 0.5, 1.0)
    matrix = symmetric + jnp.diag(diagonal_part) + 0.02 * vector[:, None] * vector[None, :]
    return matrix


def set_ends(drawn, rng, least, high):
    extent = drawn.shape
    spot = [jax.random.randint(jax.random.fold_in(rng, axis), (), 0, extent[axis]) for axis in range(len(extent))]
    drawn = drawn.at[tuple(spot)].set(least)
    longest = extent.index(max(extent))
    spot[longest] = (spot[longest] + 1) % extent[longest]
    return drawn.at[tuple(spot)].set(high)


def block_levels(key, dims, cuts, least, high):
    gain = 1.0
    for position, blocks in cuts:
        steps = jax.random.uniform(jax.random.fold_in(jax.random.fold_in(key, 6), position), (blocks,), jnp.float32, least / len(cuts), high / len(cuts))
        gain = gain * jnp.repeat(jnp.exp(steps), dims[position] // blocks).reshape((-1,) + (1,) * (len(dims) - 1 - position))
    return gain


def centred(rng, extent, deviation, most, cuts=(), held_as=jnp.bfloat16):
    result = deviation * jax.random.normal(rng, extent, jnp.float32)
    if cuts:
        result = result * block_levels(rng, extent, cuts, -0.22, 0.18)
    return jnp.clip(result, -most, most).astype(held_as)


def setup_inputs(seed: int = 0) -> dict:
    streams_of = jax.random.split(jax.random.key(seed), 7)
    return {
        "schur_tail": draw_schur_tail(jax.random.fold_in(streams_of[6], 71), 0),
        "coupling": centred(streams_of[1], (K, NL), 0.5, 4.0, ((1, 8),), jnp.float32),
        "ks_lead": centred(streams_of[2], (NL, NC), (NL + K) ** -0.5, 0.046875, ((0, 8), (1, 4)), jnp.float32),
        "ks_tail": centred(streams_of[3], (K, NC), (NL + K) ** -0.5, 0.046875, ((0, 8), (1, 4)), jnp.float32),
        "inv_mask": set_ends((jax.random.randint(streams_of[4], (K // BLK, N // BLK), 0, 2) < 1).astype(jnp.int32), jax.random.fold_in(streams_of[4], 1), 0, 1),
        "ks_mask": set_ends((jax.random.randint(streams_of[5], (N // BLK, NC // BLK), 0, 2) < 1).astype(jnp.int32), jax.random.fold_in(streams_of[5], 1), 0, 1),
    }


def expand(block_mask):
    widened = jnp.repeat(block_mask.astype(jnp.float32), BLK, axis=0)
    return jnp.repeat(widened, BLK, axis=1)

def reference(schur_tail, coupling, ks_lead, ks_tail, inv_mask, ks_mask):
    factor = jnp.linalg.cholesky(schur_tail)
    identity = jnp.eye(K, dtype=jnp.float32)
    tail_inverse = jax.scipy.linalg.solve_triangular(factor, identity, lower=True)
    lead_block = -jnp.dot(tail_inverse.astype(jnp.float32), coupling.astype(jnp.float32), precision=lax.Precision.HIGHEST, preferred_element_type=jnp.float32)
    inverse_rows = jnp.concatenate([lead_block, tail_inverse], axis=1) * expand(inv_mask)
    kohn_sham = jnp.concatenate([ks_lead, ks_tail], axis=0) * expand(ks_mask)
    return jnp.dot(inverse_rows.astype(jnp.float32), kohn_sham.astype(jnp.float32), precision=lax.Precision.HIGHEST, preferred_element_type=jnp.float32)
```

```python
import jax
import jax.numpy as jnp
from jax import lax
from jax.experimental import pallas as pl
from jax.experimental.pallas import tpu as pltpu
from jax.sharding import PartitionSpec as P

BLK = 128
SUB = 8


def expand(block_mask):
    widened = jnp.repeat(block_mask.astype(jnp.float32), BLK, axis=0)
    return jnp.repeat(widened, BLK, axis=1)


def product(left_rows, right_rows):
    return jnp.dot(
        left_rows, right_rows, precision=lax.Precision.HIGH, preferred_element_type=jnp.float32
    )


def split3(x):
    high = x.astype(jnp.bfloat16)
    rest = x - high.astype(jnp.float32)
    mid = rest.astype(jnp.bfloat16)
    low = (rest - mid.astype(jnp.float32)).astype(jnp.bfloat16)
    return high, mid, low


def dot_t(a, b):
    return lax.dot_general(a, b, (((0,), (0,)), ((), ())), preferred_element_type=jnp.float32)


def invert_block(block):
    lane = lax.broadcasted_iota(jnp.int32, (SUB, BLK), 1)
    sub = lax.broadcasted_iota(jnp.int32, (SUB, BLK), 0)
    count = BLK // SUB
    groups = [block[g * SUB : (g + 1) * SUB, :] for g in range(count)]
    done = []

    def spread(x, j):
        return jnp.broadcast_to(x[:, j : j + 1], (SUB, BLK))

    def pick(x, s):
        return jnp.broadcast_to(x[s : s + 1, :], (SUB, BLK))

    for g in range(count):
        base = g * SUB
        columns = [spread(groups[g], base + c) for c in range(SUB)]
        others = {h: [spread(groups[h], base + c) for c in range(SUB)] for h in range(g + 1, count)}
        rows = groups[g]
        final = jnp.zeros((SUB, BLK), jnp.float32)
        for s in range(SUB):
            pivot = pick(columns[s], s)
            inverse = 1.0 / pivot
            unit = jnp.where(lane == base + s, 1.0, pick(rows, s))
            final = jnp.where(sub == s, unit * lax.rsqrt(pivot), final)
            scaled = unit * inverse
            rows = jnp.where(
                sub == s, scaled, jnp.where(lane == base + s, 0.0, rows) - columns[s] * scaled
            )
            for c in range(s + 1, SUB):
                part = pick(columns[c], s) * inverse
                columns[c] = jnp.where(sub == s, part, columns[c] - columns[s] * part)
        spreads = [pick(rows, c) for c in range(SUB)]
        inside = (lane >= base) & (lane < base + SUB)
        for h in range(g + 1, count):
            first = others[h][0] * spreads[0] + others[h][1] * spreads[1]
            second = others[h][2] * spreads[2] + others[h][3] * spreads[3]
            third = others[h][4] * spreads[4] + others[h][5] * spreads[5]
            fourth = others[h][6] * spreads[6] + others[h][7] * spreads[7]
            groups[h] = jnp.where(inside, 0.0, groups[h]) - ((first + second) + (third + fourth))
        done.append(jnp.where(lane <= sub + base, final, 0.0))
    return jnp.concatenate(done, axis=0)


def inverse_kernel(a_ref, out_ref, tri_ref, wide_ref, sem):
    size = a_ref.shape[0]
    count = size // BLK
    copy = pltpu.make_async_copy(a_ref, out_ref, sem)
    copy.start()
    copy.wait()

    def step(k, carry):
        here = pl.ds(pl.multiple_of(k * BLK, BLK), BLK)
        inverse = invert_block(out_ref[here, here])
        out_ref[here, here] = jnp.zeros((BLK, BLK), jnp.float32)
        ih, im, il = split3(inverse)
        row = out_ref[here, :]
        rh, rm, rl = split3(row)
        left = jnp.concatenate([ih, im], axis=1)
        last = jnp.concatenate([ih, il], axis=1)
        new = (
            jnp.dot(last, jnp.concatenate([rl, rh], axis=0), preferred_element_type=jnp.float32)
            + jnp.dot(left, jnp.concatenate([rm, rm], axis=0), preferred_element_type=jnp.float32)
            + jnp.dot(left, jnp.concatenate([rh, rh], axis=0), preferred_element_type=jnp.float32)
        )
        out_ref[here, :] = new
        out_ref[here, here] = inverse
        full = out_ref[here, :]
        fh, fm, fl = split3(full)
        wide_ref[0:BLK, :] = fh
        wide_ref[BLK : 2 * BLK, :] = fm
        wide_ref[2 * BLK :, :] = fl

        def below(i, inner):
            there = pl.ds(pl.multiple_of(i * BLK, BLK), BLK)
            out_ref[there, here] = jnp.zeros((BLK, BLK), jnp.float32)
            ph, pm, plow = wide_ref[0:BLK, there], wide_ref[BLK : 2 * BLK, there], wide_ref[2 * BLK :, there]
            fh, fm, fl = wide_ref[0:BLK, :], wide_ref[BLK : 2 * BLK, :], wide_ref[2 * BLK :, :]
            left = jnp.concatenate([ph, pm], axis=0)
            last = jnp.concatenate([ph, plow], axis=0)
            change = (
                dot_t(last, jnp.concatenate([fl, fh], axis=0))
                + dot_t(left, jnp.concatenate([fm, fm], axis=0))
                + dot_t(left, jnp.concatenate([fh, fh], axis=0))
            )
            out_ref[there, :] = out_ref[there, :] - change
            return inner

        lax.fori_loop(k + 1, count, below, 0)
        return carry

    lax.fori_loop(0, count, step, 0)

    def clear(k, carry):
        here = pl.ds(pl.multiple_of(k * BLK, BLK), BLK)
        lane = lax.broadcasted_iota(jnp.int32, (BLK, size), 1)
        out_ref[here, :] = jnp.where(lane < (k + 1) * BLK, out_ref[here, :], 0.0)
        return carry

    lax.fori_loop(0, count, clear, 0)


def factor_inverse(gathered):
    size = gathered.shape[0]
    return pl.pallas_call(
        inverse_kernel,
        out_shape=jax.ShapeDtypeStruct((size, size), jnp.float32),
        in_specs=[pl.BlockSpec(memory_space=pl.ANY)],
        out_specs=pl.BlockSpec(memory_space=pltpu.VMEM),
        scratch_shapes=[
            pltpu.VMEM((8, BLK), jnp.float32),
            pltpu.VMEM((3 * BLK, size), jnp.bfloat16),
            pltpu.SemaphoreType.DMA(()),
        ],
        name="factor_inverse",
    )(gathered)


def per_device(schur_tail, coupling, ks_lead, ks_tail, inv_mask, ks_mask):
    row_index = lax.axis_index("row")
    col_index = lax.axis_index("col")
    gathered = lax.all_gather(schur_tail, ("row", "col"), axis=0, tiled=True)
    tail_size = gathered.shape[0]
    tail_inv = factor_inverse(gathered)
    lead_width = coupling.shape[1]
    lead_blocks = lead_width // BLK
    col_width = ks_lead.shape[1]
    col_blocks = col_width // BLK
    tail_rows = ks_tail.shape[0]
    lead_total_blocks = inv_mask.shape[1] - tail_size // BLK
    lead_mask = expand(lax.dynamic_slice_in_dim(inv_mask, row_index * lead_blocks, lead_blocks, 1))
    lead_part = -product(tail_inv, coupling) * lead_mask
    lead_ks_mask = expand(
        lax.dynamic_slice(
            ks_mask, (row_index * lead_blocks, col_index * col_blocks), (lead_blocks, col_blocks)
        )
    )
    ks_block = ks_lead * lead_ks_mask
    tail_ks_mask = expand(
        lax.dynamic_slice(
            ks_mask, (lead_total_blocks, col_index * col_blocks), (tail_size // BLK, col_blocks)
        )
    )
    masked_inv = tail_inv * expand(inv_mask[:, lead_total_blocks:])
    own_tail_mask = lax.dynamic_slice_in_dim(tail_ks_mask, row_index * tail_rows, tail_rows, 0)
    tail_block = ks_tail * own_tail_mask
    diag_cols = lax.dynamic_slice_in_dim(masked_inv, row_index * tail_rows, tail_rows, 1)
    return lax.psum_scatter(
        product(lead_part, ks_block) + product(diag_cols, tail_block),
        "row",
        scatter_dimension=0,
        tiled=True,
    )


def solution(mesh):
    in_specs = (P(("row", "col"), None), P(None, "row"), P("row", "col"), P("row", "col"), P(), P())
    out_specs = P("row", "col")
    return jax.shard_map(
        per_device, mesh=mesh, in_specs=in_specs, out_specs=out_specs, check_vma=False
    )
```

```python
import functools

import jax
import jax.numpy as jnp
from jax import lax
from jax.experimental import pallas as pl
from jax.experimental.pallas import tpu as pltpu
from jax.sharding import PartitionSpec as P

MESH = pl.DeviceIdType.MESH
BLK = 128
SUB = 8


def expand(block_mask):
    widened = jnp.repeat(block_mask.astype(jnp.float32), BLK, axis=0)
    return jnp.repeat(widened, BLK, axis=1)


def product(left_rows, right_rows):
    return jnp.dot(
        left_rows, right_rows, precision=lax.Precision.HIGH, preferred_element_type=jnp.float32
    )


def split3(x):
    high = x.astype(jnp.bfloat16)
    rest = x - high.astype(jnp.float32)
    mid = rest.astype(jnp.bfloat16)
    low = (rest - mid.astype(jnp.float32)).astype(jnp.bfloat16)
    return high, mid, low


def dot_t(a, b):
    return lax.dot_general(a, b, (((0,), (0,)), ((), ())), preferred_element_type=jnp.float32)


def invert_block(block):
    lane = lax.broadcasted_iota(jnp.int32, (SUB, BLK), 1)
    sub = lax.broadcasted_iota(jnp.int32, (SUB, BLK), 0)
    count = BLK // SUB
    groups = [block[g * SUB : (g + 1) * SUB, :] for g in range(count)]
    done = []

    def spread(x, j):
        return jnp.broadcast_to(x[:, j : j + 1], (SUB, BLK))

    def pick(x, s):
        return jnp.broadcast_to(x[s : s + 1, :], (SUB, BLK))

    for g in range(count):
        base = g * SUB
        columns = [spread(groups[g], base + c) for c in range(SUB)]
        others = {h: [spread(groups[h], base + c) for c in range(SUB)] for h in range(g + 1, count)}
        rows = groups[g]
        final = jnp.zeros((SUB, BLK), jnp.float32)
        for s in range(SUB):
            pivot = pick(columns[s], s)
            inverse = 1.0 / pivot
            unit = jnp.where(lane == base + s, 1.0, pick(rows, s))
            final = jnp.where(sub == s, unit * lax.rsqrt(pivot), final)
            scaled = unit * inverse
            rows = jnp.where(
                sub == s, scaled, jnp.where(lane == base + s, 0.0, rows) - columns[s] * scaled
            )
            for c in range(s + 1, SUB):
                part = pick(columns[c], s) * inverse
                columns[c] = jnp.where(sub == s, part, columns[c] - columns[s] * part)
        spreads = [pick(rows, c) for c in range(SUB)]
        inside = (lane >= base) & (lane < base + SUB)
        for h in range(g + 1, count):
            first = others[h][0] * spreads[0] + others[h][1] * spreads[1]
            second = others[h][2] * spreads[2] + others[h][3] * spreads[3]
            third = others[h][4] * spreads[4] + others[h][5] * spreads[5]
            fourth = others[h][6] * spreads[6] + others[h][7] * spreads[7]
            groups[h] = jnp.where(inside, 0.0, groups[h]) - ((first + second) + (third + fourth))
        done.append(jnp.where(lane <= sub + base, final, 0.0))
    return jnp.concatenate(done, axis=0)


def inverse_kernel(a_ref, out_ref, tri_ref, wide_ref, sem):
    size = a_ref.shape[0]
    count = size // BLK
    copy = pltpu.make_async_copy(a_ref, out_ref, sem)
    copy.start()
    copy.wait()

    def step(k, carry):
        here = pl.ds(pl.multiple_of(k * BLK, BLK), BLK)
        inverse = invert_block(out_ref[here, here])
        out_ref[here, here] = jnp.zeros((BLK, BLK), jnp.float32)
        ih, im, il = split3(inverse)
        row = out_ref[here, :]
        rh, rm, rl = split3(row)
        left = jnp.concatenate([ih, im], axis=1)
        last = jnp.concatenate([ih, il], axis=1)
        new = (
            jnp.dot(last, jnp.concatenate([rl, rh], axis=0), preferred_element_type=jnp.float32)
            + jnp.dot(left, jnp.concatenate([rm, rm], axis=0), preferred_element_type=jnp.float32)
            + jnp.dot(left, jnp.concatenate([rh, rh], axis=0), preferred_element_type=jnp.float32)
        )
        out_ref[here, :] = new
        out_ref[here, here] = inverse
        full = out_ref[here, :]
        fh, fm, fl = split3(full)
        wide_ref[0:BLK, :] = fh
        wide_ref[BLK : 2 * BLK, :] = fm
        wide_ref[2 * BLK :, :] = fl

        def below(i, inner):
            there = pl.ds(pl.multiple_of(i * BLK, BLK), BLK)
            out_ref[there, here] = jnp.zeros((BLK, BLK), jnp.float32)
            ph, pm, plow = wide_ref[0:BLK, there], wide_ref[BLK : 2 * BLK, there], wide_ref[2 * BLK :, there]
            fh, fm, fl = wide_ref[0:BLK, :], wide_ref[BLK : 2 * BLK, :], wide_ref[2 * BLK :, :]
            left = jnp.concatenate([ph, pm], axis=0)
            last = jnp.concatenate([ph, plow], axis=0)
            change = (
                dot_t(last, jnp.concatenate([fl, fh], axis=0))
                + dot_t(left, jnp.concatenate([fm, fm], axis=0))
                + dot_t(left, jnp.concatenate([fh, fh], axis=0))
            )
            out_ref[there, :] = out_ref[there, :] - change
            return inner

        lax.fori_loop(k + 1, count, below, 0)
        return carry

    lax.fori_loop(0, count, step, 0)

    def clear(k, carry):
        here = pl.ds(pl.multiple_of(k * BLK, BLK), BLK)
        lane = lax.broadcasted_iota(jnp.int32, (BLK, size), 1)
        out_ref[here, :] = jnp.where(lane < (k + 1) * BLK, out_ref[here, :], 0.0)
        return carry

    lax.fori_loop(0, count, clear, 0)


def factor_inverse(gathered):
    size = gathered.shape[0]
    return pl.pallas_call(
        inverse_kernel,
        out_shape=jax.ShapeDtypeStruct((size, size), jnp.float32),
        in_specs=[pl.BlockSpec(memory_space=pl.ANY)],
        out_specs=pl.BlockSpec(memory_space=pltpu.VMEM),
        scratch_shapes=[
            pltpu.VMEM((8, BLK), jnp.float32),
            pltpu.VMEM((3 * BLK, size), jnp.bfloat16),
            pltpu.SemaphoreType.DMA(()),
        ],
        name="factor_inverse",
    )(gathered)


def greet(peers):
    barrier = pltpu.get_barrier_semaphore()
    for peer in peers:
        pl.semaphore_signal(barrier, inc=1, device_id=peer, device_id_type=MESH)
    pl.semaphore_wait(barrier, len(peers))


def gather_kernel(rows, cols, x_ref, out_ref, send1, recv1, send2, recv2, send3, recv3):
    me_row, me_col = lax.axis_index("row"), lax.axis_index("col")
    chips = rows // 2
    chip, core = lax.div(me_row, 2), lax.rem(me_row, 2)
    part = x_ref.shape[0]
    whole = part * cols

    def at_chip(q):
        return q * 2 + core

    partner = (chip * 2 + 1 - core, me_col)
    col_peers = [(me_row, lax.rem(me_col + d, cols)) for d in range(1, cols)]
    chip_peers = [(at_chip(lax.rem(chip + d, chips)), me_col) for d in range(1, chips)]
    greet(col_peers + chip_peers + [partner])

    mine = out_ref.at[pl.ds(pl.multiple_of((me_row * cols + me_col) * part, SUB), part)]
    first = []
    for d in range(1, cols):
        copy = pltpu.make_async_remote_copy(
            x_ref, mine, send1.at[d - 1], recv1.at[d - 1], device_id=col_peers[d - 1], device_id_type=MESH
        )
        copy.start()
        first.append(copy)
    mine[...] = x_ref[...]
    for copy in first:
        copy.wait_recv()

    def block(row):
        return out_ref.at[pl.ds(pl.multiple_of(row * whole, SUB), whole)]

    def forward(row, slot):
        copy = pltpu.make_async_remote_copy(
            block(row), block(row), send3.at[slot], recv3.at[slot], device_id=partner, device_id_type=MESH
        )
        copy.start()
        return copy

    second = []
    for d in range(1, chips):
        copy = pltpu.make_async_remote_copy(
            block(me_row), block(me_row), send2.at[d - 1], recv2.at[d - 1],
            device_id=chip_peers[d - 1], device_id_type=MESH,
        )
        copy.start()
        second.append(copy)
    third = [forward(me_row, 0)]
    for d in range(1, chips):
        second[d - 1].wait_recv()
        third.append(forward(at_chip(lax.rem(chip + chips - d, chips)), d))
    for copy in third:
        copy.wait_recv()
    for copy in first + second + third:
        copy.wait_send()


def gather(part, mesh_rows, mesh_cols):
    dma = pltpu.SemaphoreType.DMA
    chips = mesh_rows // 2
    return pl.pallas_call(
        functools.partial(gather_kernel, mesh_rows, mesh_cols),
        out_shape=jax.ShapeDtypeStruct((part.shape[0] * mesh_rows * mesh_cols, part.shape[1]), jnp.float32),
        in_specs=[pl.BlockSpec(memory_space=pltpu.VMEM)],
        out_specs=pl.BlockSpec(memory_space=pltpu.VMEM),
        scratch_shapes=[
            dma((mesh_cols - 1,)), dma((mesh_cols - 1,)),
            dma((chips - 1,)), dma((chips - 1,)),
            dma((chips,)), dma((chips,)),
        ],
        compiler_params=pltpu.CompilerParams(collective_id=0, has_side_effects=True),
        name="gather_tail",
    )(part)


def scatter_kernel(rows, p_ref, out_ref, pair_ref, far_ref, send1, recv1, send2, recv2):
    me_row, me_col = lax.axis_index("row"), lax.axis_index("col")
    chips = rows // 2
    chip, core = lax.div(me_row, 2), lax.rem(me_row, 2)
    part = out_ref.shape[0]
    partner = (chip * 2 + 1 - core, me_col)
    targets = [lax.rem(chip + d, chips) for d in range(chips)]
    chip_peers = [(targets[d] * 2 + core, me_col) for d in range(1, chips)]
    greet(chip_peers + [partner])

    def block(row):
        return p_ref.at[pl.ds(pl.multiple_of(row * part, SUB), part)]

    order = list(range(1, chips)) + [0]
    first = {}
    for d in order:
        copy = pltpu.make_async_remote_copy(
            block(targets[d] * 2 + 1 - core), pair_ref.at[d], send1.at[d], recv1.at[d],
            device_id=partner, device_id_type=MESH,
        )
        copy.start()
        first[d] = copy
    second = []
    for d in range(1, chips):
        first[d].wait_recv()
        pair_ref[d] = pair_ref[d] + block(targets[d] * 2 + core)[...]
        copy = pltpu.make_async_remote_copy(
            pair_ref.at[d], far_ref.at[d - 1], send2.at[d - 1], recv2.at[d - 1],
            device_id=chip_peers[d - 1], device_id_type=MESH,
        )
        copy.start()
        second.append(copy)
    first[0].wait_recv()
    out_ref[...] = pair_ref[0] + block(me_row)[...]
    for d in range(1, chips):
        second[d - 1].wait_recv()
        out_ref[...] += far_ref[d - 1]
    for copy in list(first.values()) + second:
        copy.wait_send()


def scatter_sum(partial, mesh_rows):
    dma = pltpu.SemaphoreType.DMA
    chips = mesh_rows // 2
    part, width = partial.shape[0] // mesh_rows, partial.shape[1]
    return pl.pallas_call(
        functools.partial(scatter_kernel, mesh_rows),
        out_shape=jax.ShapeDtypeStruct((part, width), jnp.float32),
        in_specs=[pl.BlockSpec(memory_space=pltpu.VMEM)],
        out_specs=pl.BlockSpec(memory_space=pltpu.VMEM),
        scratch_shapes=[
            pltpu.VMEM((chips, part, width), jnp.float32),
            pltpu.VMEM((chips - 1, part, width), jnp.float32),
            dma((chips,)), dma((chips,)),
            dma((chips - 1,)), dma((chips - 1,)),
        ],
        compiler_params=pltpu.CompilerParams(collective_id=1, has_side_effects=True),
        name="scatter_sum",
    )(partial)


def per_device(mesh_rows, mesh_cols, schur_tail, coupling, ks_lead, ks_tail, inv_mask, ks_mask):
    row_index = lax.axis_index("row")
    col_index = lax.axis_index("col")
    gathered = gather(schur_tail, mesh_rows, mesh_cols)
    tail_size = gathered.shape[0]
    tail_inv = factor_inverse(gathered)
    lead_width = coupling.shape[1]
    lead_blocks = lead_width // BLK
    col_width = ks_lead.shape[1]
    col_blocks = col_width // BLK
    tail_rows = ks_tail.shape[0]
    lead_total_blocks = inv_mask.shape[1] - tail_size // BLK
    lead_mask = expand(lax.dynamic_slice_in_dim(inv_mask, row_index * lead_blocks, lead_blocks, 1))
    lead_part = -product(tail_inv, coupling) * lead_mask
    lead_ks_mask = expand(
        lax.dynamic_slice(
            ks_mask, (row_index * lead_blocks, col_index * col_blocks), (lead_blocks, col_blocks)
        )
    )
    ks_block = ks_lead * lead_ks_mask
    tail_ks_mask = expand(
        lax.dynamic_slice(
            ks_mask, (lead_total_blocks, col_index * col_blocks), (tail_size // BLK, col_blocks)
        )
    )
    masked_inv = tail_inv * expand(inv_mask[:, lead_total_blocks:])
    own_tail_mask = lax.dynamic_slice_in_dim(tail_ks_mask, row_index * tail_rows, tail_rows, 0)
    tail_block = ks_tail * own_tail_mask
    diag_cols = lax.dynamic_slice_in_dim(masked_inv, row_index * tail_rows, tail_rows, 1)
    partial = product(lead_part, ks_block) + product(diag_cols, tail_block)
    return scatter_sum(partial, mesh_rows)


def solution(mesh):
    in_specs = (P(("row", "col"), None), P(None, "row"), P("row", "col"), P("row", "col"), P(), P())
    out_specs = P("row", "col")
    return jax.shard_map(
        functools.partial(per_device, mesh.shape["row"], mesh.shape["col"]), mesh=mesh, in_specs=in_specs, out_specs=out_specs, check_vma=False
    )
```
